256 devices in a mesh: pop: 32 (over z, y_lo, core), tp: 8 (over y_hi, x).
Axes of the slice: x: 4, y: 4 (y_hi: 2, y_lo: 2; y = y_hi * 2 + y_lo), z: 8, core: 2. Of those that a mesh axis runs over, the one named last changes fastest.
Arguments:
- tokens: bfloat16 [32, 512, 1792], P('pop', None, 'tp'), may hold values from -6 to 6
- weight: bfloat16 [32, 1792, 7168], P('pop', 'tp'), may hold values from -0.125 to 0.125
- momentum: bfloat16 [32, 1792, 7168], P('pop', 'tp'), may hold values from -6 to 6
- cotangent: bfloat16 [32, 512, 7168], P('pop', None, 'tp'), may hold values from -0.5 to 0.5
- assignment: int32 [8, 2], replicated, may hold values from 0 to 31, as said below
- lr_index: int32 [32], replicated, may hold values from 0 to 7
- rates: float32 [8], replicated, may hold values from 0.01 to 0.1
Outputs:
- activation: bfloat16 [32, 512, 7168], P('pop', None, 'tp')
- new_weight: bfloat16 [32, 1792, 7168], P('pop', 'tp')
The draws below stay inside these ranges and needn't reach their ends.
Inputs may be any that keep to these rules, and one draw needn't show every extreme that they name: `assignment`: column 0 names 8 distinct members; column 1 names exactly 2 distinct members, each in some row, none of them in column 0.
All inputs are finite; a program needn't handle non-finite values.
Results may differ from the reference program's by a relative error of at most 0.015.
Values may be sent and summed in bfloat16 or wider, within the bound.
No kernel may reach another device: no remote copies, remote signals or barrier semaphores. Data moves between devices by JAX's collectives and lax.ppermute only.
A program may use at most 192 MiB of HBM per device.

```python
import math
import jax
import jax.numpy as jnp
from jax import lax

D = 1792
FF = 7168
TOK = 512
RATES = 8
MEMBERS = 32
LOSERS = 8
TOPS = 2
N_TP = 8


def draw_assignment(key, part):
    chosen_count = TOPS + LOSERS
    middle = jax.random.permutation(jax.random.fold_in(key, 11), MEMBERS - 2).astype(jnp.int32) + 1
    ends = jnp.array([0, MEMBERS - 1], dtype=jnp.int32)
    picked = jnp.concatenate([ends, middle[:chosen_count - 2]]).astype(jnp.int32)
    shuffle = jax.random.permutation(jax.random.fold_in(key, 13), chosen_count).astype(jnp.int32)
    order = picked[shuffle]
    winners_set = order[:TOPS]
    losers = order[TOPS:TOPS + LOSERS]
    picks = jax.random.randint(jax.random.fold_in(key, 12), (LOSERS,), 0, TOPS)
    rows = jnp.arange(LOSERS, dtype=jnp.int32)
    picks = jnp.where(rows < TOPS, rows, picks).astype(jnp.int32)
    winners = winners_set[picks]
    return jnp.stack([losers, winners], axis=1).astype(jnp.int32)


def plant(values, rng, low, largest):
    extent = values.shape
    place = [jax.random.randint(jax.random.fold_in(rng, axis), (), 0, extent[axis]) for axis in range(len(extent))]
    values = values.at[tuple(place)].set(low)
    longest = extent.index(max(extent))
    place[longest] = (place[longest] + 1) % extent[longest]
    return values.at[tuple(place)].set(largest)


def block_levels(rng, shape, pieces, least, high):
    loudness, own = 1.0, jax.random.fold_in(rng, 6)
    for axis_at, blocks in pieces:
        steps = jnp.exp(jax.random.uniform(jax.random.fold_in(own, axis_at), (blocks,), jnp.float32, least / len(pieces), high / len(pieces)))
        loudness = loudness * jnp.repeat(steps, shape[axis_at] // blocks).reshape([-1 if axis == axis_at else 1 for axis in range(len(shape))])
    return loudness


def centred(rng, dims, width, limit, shards=(), kind=jnp.bfloat16):
    drawn = width * jax.random.normal(rng, dims, jnp.float32)
    if shards:
        drawn = drawn * block_levels(rng, dims, shards, -0.22, 0.18)
    return jnp.clip(drawn, -limit, limit).astype(kind)


def setup_inputs(seed: int = 0) -> dict:
    arg_keys = jax.random.split(jax.random.key(seed), 8)
    return {
        "tokens": centred(arg_keys[0], (MEMBERS, TOK, D), 1.0, 6.0, ((0, 32), (2, 8))),
        "weight": centred(arg_keys[1], (MEMBERS, D, FF), D ** -0.5, 0.125, ((0, 32), (1, 8))),
        "momentum": centred(arg_keys[2], (MEMBERS, D, FF), 1.0, 6.0, ((0, 32), (1, 8))),
        "cotangent": centred(arg_keys[3], (MEMBERS, TOK, FF), 0.0625, 0.5, ((0, 32), (2, 8))),
        "assignment": draw_assignment(jax.random.fold_in(arg_keys[7], 71), 0),
        "lr_index": plant(jax.random.randint(arg_keys[5], (MEMBERS,), 0, RATES), jax.random.fold_in(arg_keys[5], 1), 0, RATES - 1).astype(jnp.int32),
        "rates": jnp.clip(jnp.exp(jax.random.uniform(arg_keys[6], (RATES,), jnp.float32, math.log(0.01), math.log(0.1))), 0.01, 0.1),
    }


def gelu_tanh(value):
    return jax.nn.gelu(value, approximate=True)

def reference(tokens, weight, momentum, cotangent, assignment, lr_index, rates):
    member_ids = jnp.arange(MEMBERS, dtype=jnp.int32)
    hit = assignment[:, 0][None, :] == member_ids[:, None]
    source_all = jnp.where(jnp.any(hit, axis=1), lax.optimization_barrier(jnp.sum(jnp.where(hit, assignment[:, 1][None, :], 0), axis=1)).astype(jnp.int32), member_ids)
    rate_ids = jnp.arange(RATES, dtype=jnp.int32)
    rate_all = lax.optimization_barrier(jnp.sum(jnp.where(rate_ids[None, :] == lr_index[:, None], rates[None, :], 0.0), axis=1))
    block = D // N_TP

    def one_member(member):
        source = source_all[member]
        inputs = tokens[member]
        taken_weight = weight[source]
        taken_momentum = momentum[source]
        hidden = jnp.zeros((TOK, FF), jnp.float32)
        for piece in range(N_TP):
            partial_value = jnp.dot(inputs[:, piece * block:(piece + 1) * block], taken_weight[piece * block:(piece + 1) * block], preferred_element_type=jnp.float32).astype(jnp.bfloat16)
            hidden = hidden + lax.optimization_barrier(partial_value).astype(jnp.float32)
        active, pullback = jax.vjp(gelu_tanh, hidden)
        grad_hidden = pullback(cotangent[member].astype(jnp.float32))[0].astype(jnp.bfloat16)
        grad_weight = jnp.dot(inputs.T, grad_hidden, preferred_element_type=jnp.float32)
        new_momentum = 0.9 * taken_momentum.astype(jnp.float32) + grad_weight
        updated = (taken_weight.astype(jnp.float32) - rate_all[member] * new_momentum).astype(jnp.bfloat16)
        return (active.astype(jnp.bfloat16), updated)
    activation, new_weight = lax.map(one_member, member_ids)
    return (activation, new_weight)
```

```python
import jax
import jax.numpy as jnp
from jax import lax
from jax.experimental import pallas as pl
from jax.experimental.pallas import tpu as pltpu
from jax.sharding import Mesh, PartitionSpec as P

POP = ("z", "yl", "c")
TP = ("yh", "x")
NZ = 8
NK = 8
GELU_A = 0.7978845608028654
GELU_B = 0.044715

MINE_A, MINE_B, THEIRS_A, THEIRS_B, CORE, LOSER, SLOT = range(7)


def params(n=1):
    return pltpu.CompilerParams(
        dimension_semantics=("arbitrary",) * n, vmem_limit_bytes=48 * 1024 * 1024
    )


def slots_kernel(tab, mine, theirs, out):
    zero = jnp.zeros(mine.shape, mine.dtype)
    m, t = mine[...], theirs[...]
    for s, (own, other) in enumerate(((MINE_A, THEIRS_A), (MINE_B, THEIRS_B))):
        out[0, s] = jnp.where(tab[own] == 1, m, jnp.where(tab[other] == 1, t, zero))


def build_slots(tab, shard, theirs):
    half, width = shard.shape[0] // 2, shard.shape[1] // NZ
    return pl.pallas_call(
        slots_kernel,
        grid_spec=pltpu.PrefetchScalarGridSpec(
            num_scalar_prefetch=1,
            grid=(NZ,),
            in_specs=[
                pl.BlockSpec((half, width), lambda j, tab: (tab[CORE], j)),
                pl.BlockSpec((half, width), lambda j, tab: (0, j)),
            ],
            out_specs=pl.BlockSpec((1, 2, half, width), lambda j, tab: (j, 0, 0, 0)),
        ),
        out_shape=jax.ShapeDtypeStruct((NZ, 2, half, width), shard.dtype),
        compiler_params=params(),
        cost_estimate=pl.CostEstimate(flops=5_000_000, bytes_accessed=10_000_000, transcendentals=0),
        name="slots",
    )(tab, shard, theirs)


def joined(tab, gathered, received):
    g, r = gathered[0, 0], received[0]
    first = tab[CORE] == 0
    return jnp.where(first, g, r), jnp.where(first, r, g)


def take_kernel(tab, own, gathered, received, out):
    half = received.shape[1]
    low, high = joined(tab, gathered, received)
    loser = tab[LOSER] == 1
    out[0, :half] = jnp.where(loser, low, own[:half])
    out[0, half:] = jnp.where(loser, high, own[half:])


def taken_specs(rows, half, width):
    return [
        pl.BlockSpec((rows, width), lambda j, tab, *_: (0, j)),
        pl.BlockSpec((1, 1, half, width), lambda j, tab, *_: (j, tab[SLOT], 0, 0)),
        pl.BlockSpec((1, half, width), lambda j, tab, *_: (j, 0, 0)),
    ]


def take(tab, shard, gathered, received):
    rows, width = shard.shape[0], shard.shape[1] // NZ
    return pl.pallas_call(
        take_kernel,
        grid_spec=pltpu.PrefetchScalarGridSpec(
            num_scalar_prefetch=1,
            grid=(NZ,),
            in_specs=taken_specs(rows, rows // 2, width),
            out_specs=pl.BlockSpec((1, rows, width), lambda j, tab: (j, 0, 0)),
        ),
        out_shape=jax.ShapeDtypeStruct((NZ, rows, width), shard.dtype),
        compiler_params=params(),
        cost_estimate=pl.CostEstimate(flops=5_000_000, bytes_accessed=10_000_000, transcendentals=0),
        name="take",
    )(tab, shard, gathered, received)


def final_kernel(tab, rate, own, gathered, received, back, out):
    half = received.shape[1]
    low, high = joined(tab, gathered, received)
    loser = tab[LOSER] == 1
    scale = 0.9 * rate[0]
    for at, piece in ((0, low), (half, high)):
        rows = pl.ds(at, half)
        m = jnp.where(loser, piece, own[rows]).astype(jnp.float32)
        out[rows] = (back[0, rows].astype(jnp.float32) - scale * m).astype(out.dtype)


def final(tab, rate, shard, gathered, received, back):
    rows, width = shard.shape[0], shard.shape[1] // NZ
    return pl.pallas_call(
        final_kernel,
        grid_spec=pltpu.PrefetchScalarGridSpec(
            num_scalar_prefetch=2,
            grid=(NZ,),
            in_specs=taken_specs(rows, rows // 2, width)
            + [pl.BlockSpec((1, rows, width), lambda j, tab, rate: (j, 0, 0))],
            out_specs=pl.BlockSpec((rows, width), lambda j, tab, rate: (0, j)),
        ),
        out_shape=jax.ShapeDtypeStruct(shard.shape, shard.dtype),
        compiler_params=params(),
        cost_estimate=pl.CostEstimate(flops=5_000_000, bytes_accessed=13_000_000, transcendentals=0),
        name="final",
    )(tab, rate, shard, gathered, received, back)


def step_kernel(rate, tokens, weight, cot, act, back, acc, grad):
    i = pl.program_id(0)

    @pl.when(i == 0)
    def _():
        acc[...] = jnp.zeros_like(acc)

    @pl.when(i < NK)
    def _():
        acc[...] += lax.dot_general(
            tokens[0], weight[0], (((0,), (0,)), ((), ())), preferred_element_type=jnp.float32
        )

    @pl.when(i == NK - 1)
    def _():
        v = acc[...]
        t = jnp.tanh(GELU_A * (v + GELU_B * (v * v * v)))
        act[...] = (0.5 * v * (1.0 + t)).astype(act.dtype)
        slope = 0.5 * (1.0 + t) + 0.5 * v * (1.0 - t * t) * (GELU_A * (1.0 + 3.0 * GELU_B * (v * v)))
        grad[...] = (cot[...].astype(jnp.float32) * slope).astype(grad.dtype)

    @pl.when(i >= NK)
    def _():
        gw = jnp.dot(tokens[0], grad[...], preferred_element_type=jnp.float32)
        back[0] = (weight[0].astype(jnp.float32) - rate[0] * gw).astype(back.dtype)


def step(rate, tokens, weight, cot):
    nk, r, t = tokens.shape
    f = weight.shape[2]
    return pl.pallas_call(
        step_kernel,
        grid_spec=pltpu.PrefetchScalarGridSpec(
            num_scalar_prefetch=1,
            grid=(2 * NK,),
            in_specs=[
                pl.BlockSpec((1, r, t), lambda i, rate: (lax.rem(i, NK), 0, 0)),
                pl.BlockSpec((1, r, f), lambda i, rate: (lax.rem(i, NK), 0, 0)),
                pl.BlockSpec((t, f), lambda i, rate: (0, 0)),
            ],
            out_specs=[
                pl.BlockSpec((t, f), lambda i, rate: (0, 0)),
                pl.BlockSpec((1, r, f), lambda i, rate: (jnp.maximum(i - NK, 0), 0, 0)),
            ],
            scratch_shapes=[pltpu.VMEM((t, f), jnp.float32), pltpu.VMEM((t, f), jnp.bfloat16)],
        ),
        out_shape=[
            jax.ShapeDtypeStruct((t, f), jnp.bfloat16),
            jax.ShapeDtypeStruct((nk, r, f), jnp.bfloat16),
        ],
        compiler_params=params(),
        cost_estimate=pl.CostEstimate(
            flops=4 * nk * t * r * f, bytes_accessed=20_000_000, transcendentals=t * f
        ),
        name="step",
    )(rate, tokens, weight, cot)


def swap_core(x):
    return lax.ppermute(x, "c", [(0, 1), (1, 0)])


def own_slots(tab, shard, core):
    half = shard.shape[0] // 2
    theirs = swap_core(lax.dynamic_slice_in_dim(shard, (1 - core) * half, half, axis=0))
    return build_slots(tab, shard, theirs)


def scatter(slots):
    return lax.psum_scatter(slots, "z", scatter_dimension=0, tiled=True)


def gather(mine):
    mine = mine + lax.ppermute(mine, "yl", [(0, 1), (1, 0)])
    return lax.all_gather(mine, "z", axis=0, tiled=True)


def other_half(gathered, slot):
    return swap_core(lax.dynamic_index_in_dim(gathered, slot, axis=1, keepdims=False))


def local(tokens, weight, momentum, cotangent, assignment, lr_index, rates):
    core = lax.axis_index("c")
    me = lax.axis_index(POP)
    partner = me + 1 - 2 * core
    loser_ids, winner_ids = assignment[:, 0], assignment[:, 1]
    win_a, win_b = jnp.min(winner_ids), jnp.max(winner_ids)

    def slot_of(member):
        hit = loser_ids == member
        return jnp.any(hit), jnp.any(hit & (winner_ids == win_b)).astype(jnp.int32)

    loser, slot = slot_of(me)
    _, partner_slot = slot_of(partner)
    tab = jnp.stack(
        [
            (win_a == me).astype(jnp.int32),
            (win_b == me).astype(jnp.int32),
            (win_a == partner).astype(jnp.int32),
            (win_b == partner).astype(jnp.int32),
            core.astype(jnp.int32),
            loser.astype(jnp.int32),
            slot,
        ]
    )
    member_ids = jnp.arange(lr_index.shape[0], dtype=jnp.int32)
    my_index = jnp.sum(jnp.where(member_ids == me, lr_index, 0))
    rate_ids = jnp.arange(rates.shape[0], dtype=jnp.int32)
    rate = jnp.sum(jnp.where(rate_ids == my_index, rates, 0.0)).reshape(1)

    w, m = weight[0], momentum[0]
    w_slots, m_slots = own_slots(tab, w, core), own_slots(tab, m, core)
    turned = jnp.swapaxes(tokens, 1, 2)
    all_tokens = lax.all_to_all(
        jnp.broadcast_to(turned, (NK,) + turned.shape[1:]), TP, 0, 0, tiled=True
    )
    w_mine, all_tokens = lax.optimization_barrier((scatter(w_slots), all_tokens))
    w_won = gather(w_mine)
    m_slots, w_won = lax.optimization_barrier((m_slots, w_won))
    m_mine = scatter(m_slots)
    w_taken = take(tab, w, w_won, other_half(w_won, partner_slot))
    w_columns = lax.all_to_all(w_taken, TP, 0, 0, tiled=True)
    m_mine, w_columns = lax.optimization_barrier((m_mine, w_columns))
    m_won = gather(m_mine)
    activation, back = step(rate, all_tokens, w_columns, cotangent[0])
    back = lax.all_to_all(back, TP, 0, 0, tiled=True)
    updated = final(tab, rate, m, m_won, other_half(m_won, partner_slot), back)
    return (activation[None], updated[None])


def solution(mesh):
    fine = Mesh(mesh.devices.reshape(8, 2, 2, 2, 4), POP + TP)
    placed = (
        P(POP, None, TP),
        P(POP, TP, None),
        P(POP, TP, None),
        P(POP, None, TP),
        P(),
        P(),
        P(),
    )
    return jax.shard_map(
        local,
        mesh=fine,
        in_specs=placed,
        out_specs=(P(POP, None, TP), P(POP, TP, None)),
        check_vma=False,
    )
```

```python
import jax
import jax.numpy as jnp
from jax import lax
from jax.experimental import pallas as pl
from jax.experimental.pallas import tpu as pltpu
from jax.sharding import Mesh, PartitionSpec as P

POP = ("z", "yl", "c")
TP = ("yh", "x")
NZ = 8
NK = 8
ROWS = 16
PAIR = 2
GELU_A = 0.7978845608028654
GELU_B = 0.044715

MINE_A, MINE_B, THEIRS_A, THEIRS_B, CORE, LOSER, SLOT, PLANE = range(8)
DISTANCES = (0, -1, 1, -2, 2, -3, 3, 4)


def params(n=1):
    return pltpu.CompilerParams(
        dimension_semantics=("arbitrary",) * n, vmem_limit_bytes=48 * 1024 * 1024
    )


def slots_kernel(tab, mine, theirs, out):
    pair, _, half, width = out.shape
    zero = jnp.zeros((half, width), mine.dtype)
    for j in range(pair):
        at = slice(j * width, (j + 1) * width)
        for s, (own, other) in enumerate(((MINE_A, THEIRS_A), (MINE_B, THEIRS_B))):
            out[j, s] = jnp.where(
                tab[own] == 1, mine[:, at], jnp.where(tab[other] == 1, theirs[:, at], zero)
            )


def build_slots(tab, shard, theirs):
    half, width = shard.shape[0] // 2, shard.shape[1] // NZ
    return pl.pallas_call(
        slots_kernel,
        grid_spec=pltpu.PrefetchScalarGridSpec(
            num_scalar_prefetch=1,
            grid=(NZ // PAIR,),
            in_specs=[
                pl.BlockSpec((half, PAIR * width), lambda j, tab: (tab[CORE], j)),
                pl.BlockSpec((half, PAIR * width), lambda j, tab: (0, j)),
            ],
            out_specs=pl.BlockSpec((PAIR, 2, half, width), lambda j, tab: (j, 0, 0, 0)),
        ),
        out_shape=jax.ShapeDtypeStruct((NZ, 2, half, width), shard.dtype),
        compiler_params=params(),
        cost_estimate=pl.CostEstimate(flops=5_000_000, bytes_accessed=10_000_000, transcendentals=0),
        name="slots",
    )(tab, shard, theirs)


def row_slots_kernel(tab, mine, theirs, out):
    nz, pair, _, rows, width = out.shape
    zero = jnp.zeros((rows, width), out.dtype)
    for k in range(pair):
        for z in range(nz - 1):
            at = slice(z * rows, (z + 1) * rows), slice(k * width, (k + 1) * width)
            for s, (own, other) in enumerate(((MINE_A, THEIRS_A), (MINE_B, THEIRS_B))):
                out[z, k, s] = jnp.where(
                    tab[own] == 1, mine[at], jnp.where(tab[other] == 1, theirs[at], zero)
                )
        for s in range(2):
            out[nz - 1, k, s] = zero


def build_row_slots(tab, shard, theirs):
    half, width = shard.shape[0] // 2, shard.shape[1] // NK
    rows = half // (NZ - 1)
    return pl.pallas_call(
        row_slots_kernel,
        grid_spec=pltpu.PrefetchScalarGridSpec(
            num_scalar_prefetch=1,
            grid=(NK // PAIR,),
            in_specs=[
                pl.BlockSpec((half, PAIR * width), lambda j, tab: (tab[CORE], j)),
                pl.BlockSpec((half, PAIR * width), lambda j, tab: (0, j)),
            ],
            out_specs=pl.BlockSpec((NZ, PAIR, 2, rows, width), lambda j, tab: (0, j, 0, 0, 0)),
        ),
        out_shape=jax.ShapeDtypeStruct((NZ, NK, 2, rows, width), shard.dtype),
        compiler_params=params(),
        cost_estimate=pl.CostEstimate(flops=5_000_000, bytes_accessed=10_000_000, transcendentals=0),
        name="row_slots",
    )(tab, shard, theirs)


def copy_kernel(x, out):
    width = out.shape[2]
    for k in range(out.shape[0]):
        out[k] = x[:, k * width : (k + 1) * width]


def column_blocks(shard):
    rows, width = shard.shape[0], shard.shape[1] // NK
    return pl.pallas_call(
        copy_kernel,
        grid=(NK // 2,),
        in_specs=[pl.BlockSpec((rows, 2 * width), lambda j: (0, j))],
        out_specs=pl.BlockSpec((2, rows, width), lambda j: (j, 0, 0)),
        out_shape=jax.ShapeDtypeStruct((NK, rows, width), shard.dtype),
        compiler_params=params(),
        cost_estimate=pl.CostEstimate(flops=1_000_000, bytes_accessed=6_400_000, transcendentals=0),
        name="column_blocks",
    )(shard)


def final_kernel(tab, rate, own, gathered, received, back, out):
    half, width = received.shape[1:]
    scale = 0.9 * rate[0]
    loser, first = tab[LOSER] == 1, tab[CORE] == 0

    def rows_of(at, low):
        def body(i, carry):
            here = pl.ds(pl.multiple_of(i * ROWS, ROWS), ROWS)
            there = pl.ds(pl.multiple_of(at + i * ROWS, ROWS), ROWS)
            for j in range(PAIR):
                at_j = pl.ds(j * width, width)
                g, r = gathered[j, 0, here], received[j, here]
                m = jnp.where(loser, jnp.where(low, g, r), own[there, at_j]).astype(jnp.float32)
                out[there, at_j] = (back[j, there].astype(jnp.float32) - scale * m).astype(out.dtype)
            return carry

        lax.fori_loop(0, half // ROWS, body, 0, unroll=True)

    rows_of(0, first)
    rows_of(half, jnp.logical_not(first))


def final(tab, rate, shard, gathered, received, back):
    rows, width = shard.shape[0], shard.shape[1] // NZ
    half = rows // 2
    return pl.pallas_call(
        final_kernel,
        grid_spec=pltpu.PrefetchScalarGridSpec(
            num_scalar_prefetch=2,
            grid=(NZ // PAIR,),
            in_specs=[
                pl.BlockSpec((rows, PAIR * width), lambda j, tab, rate: (0, j)),
                pl.BlockSpec((PAIR, 1, half, width), lambda j, tab, rate: (j, tab[SLOT], 0, 0)),
                pl.BlockSpec((PAIR, half, width), lambda j, tab, rate: (j, 0, 0)),
                pl.BlockSpec((PAIR, rows, width), lambda j, tab, rate: (j, 0, 0)),
            ],
            out_specs=pl.BlockSpec((rows, PAIR * width), lambda j, tab, rate: (0, j)),
        ),
        out_shape=jax.ShapeDtypeStruct(shard.shape, shard.dtype),
        compiler_params=params(),
        cost_estimate=pl.CostEstimate(flops=5_000_000, bytes_accessed=13_000_000, transcendentals=0),
        name="final",
    )(tab, rate, shard, gathered, received, back)


def step_kernel(tab, rate, tokens, own, cot, received, *refs):
    gathered, (act, back, acc, grad, weight) = refs[: len(DISTANCES)], refs[len(DISTANCES) :]
    i = pl.program_id(0)
    steps = NK // PAIR
    pair = lax.rem(i, steps) * PAIR
    half = own.shape[1] // 2
    width = own.shape[2]

    @pl.when(i < steps)
    def _():
        weight[pl.ds(pair, PAIR)] = own[...]
        for n, distance in enumerate(DISTANCES):
            plane = lax.rem(tab[PLANE] + NZ + distance, NZ)

            @pl.when((tab[LOSER] == 1) & (plane < NZ - 1))
            def _():
                near = pl.multiple_of(tab[CORE] * half + plane * ROWS, ROWS)
                far = pl.multiple_of((1 - tab[CORE]) * half + plane * ROWS, ROWS)
                for p in range(PAIR):
                    weight[pair + p, pl.ds(near, ROWS)] = gathered[n][p, 0]
                    weight[pair + p, pl.ds(far, ROWS)] = received[n, p]

        t = tokens[pl.ds(pair, PAIR)].reshape(PAIR * 2 * half, -1)
        w = weight[pl.ds(pair, PAIR)].reshape(PAIR * 2 * half, width)
        part = lax.dot_general(t, w, (((0,), (0,)), ((), ())), preferred_element_type=jnp.float32)

        @pl.when(i == 0)
        def _():
            acc[...] = part

        @pl.when(i > 0)
        def _():
            acc[...] += part

    @pl.when(i == steps - 1)
    def _():
        def body(c, carry):
            rows = pl.ds(pl.multiple_of(c * ROWS, ROWS), ROWS)
            v = acc[rows]
            vv = v * v
            t = jnp.tanh(v * (GELU_A + (GELU_A * GELU_B) * vv))
            up = 0.5 + 0.5 * t
            act[rows] = (v * up).astype(act.dtype)
            slope = up + v * (1.0 - t * t) * (0.5 * GELU_A + (1.5 * GELU_A * GELU_B) * vv)
            grad[rows] = (cot[rows].astype(jnp.float32) * slope).astype(grad.dtype)
            return carry

        lax.fori_loop(0, acc.shape[0] // ROWS, body, 0, unroll=2)

    @pl.when(i >= steps)
    def _():
        t = tokens[pl.ds(pair, PAIR)].reshape(PAIR * 2 * half, -1)
        gw = jnp.dot(t, grad[...], preferred_element_type=jnp.float32)
        w = weight[pl.ds(pair, PAIR)].reshape(PAIR * 2 * half, width)
        back[...] = (w.astype(jnp.float32) - rate[0] * gw).astype(back.dtype).reshape(back.shape)


def step(tab, rate, tokens, own, cot, received, gathered):
    nk, r, t = tokens.shape
    f = own.shape[2]
    pieces, rows = received.shape[0], received.shape[2]
    steps = NK // PAIR

    def at(i):
        return jnp.minimum(i, steps - 1)

    return pl.pallas_call(
        step_kernel,
        grid_spec=pltpu.PrefetchScalarGridSpec(
            num_scalar_prefetch=2,
            grid=(2 * steps,),
            in_specs=[
                pl.BlockSpec((nk, r, t), lambda i, tab, rate: (0, 0, 0)),
                pl.BlockSpec((PAIR, r, f), lambda i, tab, rate: (at(i), 0, 0)),
                pl.BlockSpec((t, f), lambda i, tab, rate: (0, 0)),
                pl.BlockSpec((pieces, PAIR, rows, f), lambda i, tab, rate: (0, at(i), 0, 0)),
            ]
            + [pl.BlockSpec((PAIR, 1, rows, f), lambda i, tab, rate: (at(i), tab[SLOT], 0, 0))] * pieces,
            out_specs=[
                pl.BlockSpec((t, f), lambda i, tab, rate: (0, 0)),
                pl.BlockSpec((PAIR, r, f), lambda i, tab, rate: (jnp.maximum(i - steps, 0), 0, 0)),
            ],
            scratch_shapes=[
                pltpu.VMEM((t, f), jnp.float32),
                pltpu.VMEM((t, f), jnp.bfloat16),
                pltpu.VMEM((nk, r, f), jnp.bfloat16),
            ],
        ),
        out_shape=[
            jax.ShapeDtypeStruct((t, f), jnp.bfloat16),
            jax.ShapeDtypeStruct((nk, r, f), jnp.bfloat16),
        ],
        compiler_params=params(),
        cost_estimate=pl.CostEstimate(
            flops=4 * nk * t * r * f, bytes_accessed=20_000_000, transcendentals=t * f
        ),
        name="step",
    )(tab, rate, tokens, own, cot, received, *gathered)


def swap_core(x):
    return lax.ppermute(x, "c", [(0, 1), (1, 0)])


def swap_column(x):
    return lax.ppermute(x, "yl", [(0, 1), (1, 0)])


def partner_rows(shard, core):
    half = shard.shape[0] // 2
    return swap_core(lax.dynamic_slice_in_dim(shard, (1 - core) * half, half, axis=0))


def scatter(slots):
    return lax.psum_scatter(slots, "z", scatter_dimension=0, tiled=True)


def gather(mine):
    return lax.all_gather(mine, "z", axis=0, tiled=True)


def ring(piece):
    up = [(z, (z + 1) % NZ) for z in range(NZ)]
    down = [(z, (z - 1) % NZ) for z in range(NZ)]
    low = high = piece
    pieces = [piece]
    for _ in range(NZ // 2 - 1):
        low, high = lax.ppermute(low, "z", up), lax.ppermute(high, "z", down)
        pieces += [low, high]
    half = piece.shape[0] // 2
    last = lax.ppermute(low[:half], "z", up), lax.ppermute(high[half:], "z", down)
    return pieces + [jnp.concatenate(last)]


def local(tokens, weight, momentum, cotangent, assignment, lr_index, rates):
    core = lax.axis_index("c")
    me = lax.axis_index(POP)
    partner = me + 1 - 2 * core
    loser_ids, winner_ids = assignment[:, 0], assignment[:, 1]
    win_a, win_b = jnp.min(winner_ids), jnp.max(winner_ids)

    def slot_of(member):
        hit = loser_ids == member
        return jnp.any(hit), jnp.any(hit & (winner_ids == win_b)).astype(jnp.int32)

    loser, slot = slot_of(me)
    _, partner_slot = slot_of(partner)
    tab = jnp.stack(
        [
            (win_a == me).astype(jnp.int32),
            (win_b == me).astype(jnp.int32),
            (win_a == partner).astype(jnp.int32),
            (win_b == partner).astype(jnp.int32),
            core.astype(jnp.int32),
            loser.astype(jnp.int32),
            slot,
            lax.axis_index("z").astype(jnp.int32),
        ]
    )
    member_ids = jnp.arange(lr_index.shape[0], dtype=jnp.int32)
    my_index = jnp.sum(jnp.where(member_ids == me, lr_index, 0))
    rate_ids = jnp.arange(rates.shape[0], dtype=jnp.int32)
    rate = jnp.sum(jnp.where(rate_ids == my_index, rates, 0.0)).reshape(1)

    w, m = weight[0], momentum[0]
    w_slots = build_row_slots(tab, w, partner_rows(w, core))
    w_mine = scatter(w_slots)
    own_columns = lax.all_to_all(column_blocks(w), TP, 0, 0, tiled=True)
    m_slots = build_slots(tab, m, partner_rows(m, core))
    w_mine, own_columns, m_slots = lax.optimization_barrier((w_mine, own_columns, m_slots))
    m_mine = scatter(m_slots)
    both = jnp.broadcast_to(w_mine, (2,) + w_mine.shape[1:])
    both = both.reshape((2 * NK,) + w_mine.shape[2:])
    both = lax.all_to_all(both, ("yl",) + TP, 0, 0, tiled=True)
    w_mine = both[:NK] + both[NK:]
    turned = jnp.swapaxes(tokens, 1, 2)
    w_mine, turned = lax.optimization_barrier((w_mine, turned))
    all_tokens = lax.all_to_all(
        jnp.broadcast_to(turned, (NK,) + turned.shape[1:]), TP, 0, 0, tiled=True
    )
    pieces = ring(w_mine)
    pieces[-1], m_mine, all_tokens = lax.optimization_barrier((pieces[-1], m_mine, all_tokens))
    w_other = swap_core(
        jnp.stack(
            [lax.dynamic_index_in_dim(p, partner_slot, axis=1, keepdims=False) for p in pieces]
        )
    )
    m_across, w_other = lax.optimization_barrier((swap_column(m_mine), w_other))
    m_won = gather(m_mine + m_across)
    activation, back = step(tab, rate, all_tokens, own_columns, cotangent[0], w_other, pieces)
    back = lax.all_to_all(back, TP, 0, 0, tiled=True)
    m_other = swap_core(lax.dynamic_index_in_dim(m_won, partner_slot, axis=1, keepdims=False))
    updated = final(tab, rate, m, m_won, m_other, back)
    return (activation[None], updated[None])


def solution(mesh):
    fine = Mesh(mesh.devices.reshape(8, 2, 2, 2, 4), POP + TP)
    placed = (
        P(POP, None, TP),
        P(POP, TP, None),
        P(POP, TP, None),
        P(POP, None, TP),
        P(),
        P(),
        P(),
    )
    return jax.shard_map(
        local,
        mesh=fine,
        in_specs=placed,
        out_specs=(P(POP, None, TP), P(POP, TP, None)),
        check_vma=False,
    )
```

```python
import jax
import jax.numpy as jnp
from jax import lax
from jax.experimental import pallas as pl
from jax.experimental.pallas import tpu as pltpu
from jax.sharding import Mesh, PartitionSpec as P

POP = ("z", "yl", "c")
TP = ("yh", "x")
NZ = 8
NK = 8
ROWS = 16
PAIR = 2
GELU_A = 0.7978845608028654
GELU_B = 0.044715

MINE_A, MINE_B, THEIRS_A, THEIRS_B, CORE, LOSER, SLOT, PLANE = range(8)
DISTANCES = (0, -1, 1, -2, 2, -3, 3, 4)


def params(n=1):
    return pltpu.CompilerParams(
        dimension_semantics=("arbitrary",) * n, vmem_limit_bytes=48 * 1024 * 1024
    )


def slots_kernel(tab, mine, theirs, out):
    pair, _, half, width = out.shape
    zero = jnp.zeros((half, width), mine.dtype)
    for j in range(pair):
        at = slice(j * width, (j + 1) * width)
        for s, (own, other) in enumerate(((MINE_A, THEIRS_A), (MINE_B, THEIRS_B))):
            out[j, s] = jnp.where(
                tab[own] == 1, mine[:, at], jnp.where(tab[other] == 1, theirs[:, at], zero)
            )


def build_slots(tab, shard, theirs):
    half, width = shard.shape[0] // 2, shard.shape[1] // NZ
    return pl.pallas_call(
        slots_kernel,
        grid_spec=pltpu.PrefetchScalarGridSpec(
            num_scalar_prefetch=1,
            grid=(NZ // PAIR,),
            in_specs=[
                pl.BlockSpec((half, PAIR * width), lambda j, tab: (tab[CORE], j)),
                pl.BlockSpec((half, PAIR * width), lambda j, tab: (0, j)),
            ],
            out_specs=pl.BlockSpec((PAIR, 2, half, width), lambda j, tab: (j, 0, 0, 0)),
        ),
        out_shape=jax.ShapeDtypeStruct((NZ, 2, half, width), shard.dtype),
        compiler_params=params(),
        cost_estimate=pl.CostEstimate(flops=5_000_000, bytes_accessed=10_000_000, transcendentals=0),
        name="slots",
    )(tab, shard, theirs)


def row_slots_kernel(tab, mine, theirs, out):
    nz, pair, _, rows, width = out.shape
    zero = jnp.zeros((rows, width), out.dtype)
    for k in range(pair):
        for z in range(nz - 1):
            at = slice(z * rows, (z + 1) * rows), slice(k * width, (k + 1) * width)
            for s, (own, other) in enumerate(((MINE_A, THEIRS_A), (MINE_B, THEIRS_B))):
                out[z, k, s] = jnp.where(
                    tab[own] == 1, mine[at], jnp.where(tab[other] == 1, theirs[at], zero)
                )
        for s in range(2):
            out[nz - 1, k, s] = zero


def build_row_slots(tab, shard, theirs):
    half, width = shard.shape[0] // 2, shard.shape[1] // NK
    rows = half // (NZ - 1)
    return pl.pallas_call(
        row_slots_kernel,
        grid_spec=pltpu.PrefetchScalarGridSpec(
            num_scalar_prefetch=1,
            grid=(NK // PAIR,),
            in_specs=[
                pl.BlockSpec((half, PAIR * width), lambda j, tab: (tab[CORE], j)),
                pl.BlockSpec((half, PAIR * width), lambda j, tab: (0, j)),
            ],
            out_specs=pl.BlockSpec((NZ, PAIR, 2, rows, width), lambda j, tab: (0, j, 0, 0, 0)),
        ),
        out_shape=jax.ShapeDtypeStruct((NZ, NK, 2, rows, width), shard.dtype),
        compiler_params=params(),
        cost_estimate=pl.CostEstimate(flops=5_000_000, bytes_accessed=10_000_000, transcendentals=0),
        name="row_slots",
    )(tab, shard, theirs)


def copy_kernel(x, out):
    width = out.shape[2]
    for k in range(out.shape[0]):
        out[k] = x[:, k * width : (k + 1) * width]


def column_blocks(shard):
    rows, width = shard.shape[0], shard.shape[1] // NK
    return pl.pallas_call(
        copy_kernel,
        grid=(NK // 2,),
        in_specs=[pl.BlockSpec((rows, 2 * width), lambda j: (0, j))],
        out_specs=pl.BlockSpec((2, rows, width), lambda j: (j, 0, 0)),
        out_shape=jax.ShapeDtypeStruct((NK, rows, width), shard.dtype),
        compiler_params=params(),
        cost_estimate=pl.CostEstimate(flops=1_000_000, bytes_accessed=6_400_000, transcendentals=0),
        name="column_blocks",
    )(shard)


def final_kernel(tab, rate, own, gathered, received, back, out):
    half, width = received.shape[1:]
    scale = 0.9 * rate[0]
    loser, first = tab[LOSER] == 1, tab[CORE] == 0

    def rows_of(at, low):
        def body(i, carry):
            here = pl.ds(pl.multiple_of(i * ROWS, ROWS), ROWS)
            there = pl.ds(pl.multiple_of(at + i * ROWS, ROWS), ROWS)
            for j in range(PAIR):
                at_j = pl.ds(j * width, width)
                g, r = gathered[j, 0, here], received[j, here]
                m = jnp.where(loser, jnp.where(low, g, r), own[there, at_j]).astype(jnp.float32)
                out[there, at_j] = (back[j, there].astype(jnp.float32) - scale * m).astype(out.dtype)
            return carry

        lax.fori_loop(0, half // ROWS, body, 0, unroll=True)

    rows_of(0, first)
    rows_of(half, jnp.logical_not(first))


def final(tab, rate, shard, gathered, received, back):
    rows, width = shard.shape[0], shard.shape[1] // NZ
    half = rows // 2
    return pl.pallas_call(
        final_kernel,
        grid_spec=pltpu.PrefetchScalarGridSpec(
            num_scalar_prefetch=2,
            grid=(NZ // PAIR,),
            in_specs=[
                pl.BlockSpec((rows, PAIR * width), lambda j, tab, rate: (0, j)),
                pl.BlockSpec((PAIR, 1, half, width), lambda j, tab, rate: (j, tab[SLOT], 0, 0)),
                pl.BlockSpec((PAIR, half, width), lambda j, tab, rate: (j, 0, 0)),
                pl.BlockSpec((PAIR, rows, width), lambda j, tab, rate: (j, 0, 0)),
            ],
            out_specs=pl.BlockSpec((rows, PAIR * width), lambda j, tab, rate: (0, j)),
        ),
        out_shape=jax.ShapeDtypeStruct(shard.shape, shard.dtype),
        compiler_params=params(),
        cost_estimate=pl.CostEstimate(flops=5_000_000, bytes_accessed=13_000_000, transcendentals=0),
        name="final",
    )(tab, rate, shard, gathered, received, back)


def step_kernel(tab, rate, tokens, own, cot, received, *refs):
    gathered, (act, back, acc, grad, weight) = refs[: len(DISTANCES)], refs[len(DISTANCES) :]
    i = pl.program_id(0)
    steps = NK // PAIR
    pair = lax.rem(i, steps) * PAIR
    half = own.shape[1] // 2
    width = own.shape[2]

    @pl.when(i < steps)
    def _():
        weight[pl.ds(pair, PAIR)] = own[...]
        for n, distance in enumerate(DISTANCES):
            plane = lax.rem(tab[PLANE] + NZ + distance, NZ)

            @pl.when((tab[LOSER] == 1) & (plane < NZ - 1))
            def _():
                near = pl.multiple_of(tab[CORE] * half + plane * ROWS, ROWS)
                far = pl.multiple_of((1 - tab[CORE]) * half + plane * ROWS, ROWS)
                for p in range(PAIR):
                    weight[pair + p, pl.ds(near, ROWS)] = gathered[n][p, 0]
                    weight[pair + p, pl.ds(far, ROWS)] = received[n, p]

        t = tokens[pl.ds(pair, PAIR)].reshape(PAIR * 2 * half, -1)
        w = weight[pl.ds(pair, PAIR)].reshape(PAIR * 2 * half, width)
        part = lax.dot_general(t, w, (((0,), (0,)), ((), ())), preferred_element_type=jnp.float32)

        @pl.when(i == 0)
        def _():
            acc[...] = part

        @pl.when(i > 0)
        def _():
            acc[...] += part

    @pl.when(i == steps - 1)
    def _():
        def body(c, carry):
            rows = pl.ds(pl.multiple_of(c * ROWS, ROWS), ROWS)
            v = acc[rows]
            vv = v * v
            t = jnp.tanh(v * (GELU_A + (GELU_A * GELU_B) * vv))
            up = 0.5 + 0.5 * t
            act[rows] = (v * up).astype(act.dtype)
            slope = up + v * (1.0 - t * t) * (0.5 * GELU_A + (1.5 * GELU_A * GELU_B) * vv)
            grad[rows] = (cot[rows].astype(jnp.float32) * slope).astype(grad.dtype)
            return carry

        lax.fori_loop(0, acc.shape[0] // ROWS, body, 0, unroll=2)

    @pl.when(i >= steps)
    def _():
        t = tokens[pl.ds(pair, PAIR)].reshape(PAIR * 2 * half, -1)
        gw = jnp.dot(t, grad[...], preferred_element_type=jnp.float32)
        w = weight[pl.ds(pair, PAIR)].reshape(PAIR * 2 * half, width)
        back[...] = (w.astype(jnp.float32) - rate[0] * gw).astype(back.dtype).reshape(back.shape)


def step(tab, rate, tokens, own, cot, received, gathered):
    nk, r, t = tokens.shape
    f = own.shape[2]
    pieces, rows = received.shape[0], received.shape[2]
    steps = NK // PAIR

    def at(i):
        return jnp.minimum(i, steps - 1)

    return pl.pallas_call(
        step_kernel,
        grid_spec=pltpu.PrefetchScalarGridSpec(
            num_scalar_prefetch=2,
            grid=(2 * steps,),
            in_specs=[
                pl.BlockSpec((nk, r, t), lambda i, tab, rate: (0, 0, 0)),
                pl.BlockSpec((PAIR, r, f), lambda i, tab, rate: (at(i), 0, 0)),
                pl.BlockSpec((t, f), lambda i, tab, rate: (0, 0)),
                pl.BlockSpec((pieces, PAIR, rows, f), lambda i, tab, rate: (0, at(i), 0, 0)),
            ]
            + [pl.BlockSpec((PAIR, 1, rows, f), lambda i, tab, rate: (at(i), tab[SLOT], 0, 0))] * pieces,
            out_specs=[
                pl.BlockSpec((t, f), lambda i, tab, rate: (0, 0)),
                pl.BlockSpec((PAIR, r, f), lambda i, tab, rate: (jnp.maximum(i - steps, 0), 0, 0)),
            ],
            scratch_shapes=[
                pltpu.VMEM((t, f), jnp.float32),
                pltpu.VMEM((t, f), jnp.bfloat16),
                pltpu.VMEM((nk, r, f), jnp.bfloat16),
            ],
        ),
        out_shape=[
            jax.ShapeDtypeStruct((t, f), jnp.bfloat16),
            jax.ShapeDtypeStruct((nk, r, f), jnp.bfloat16),
        ],
        compiler_params=params(),
        cost_estimate=pl.CostEstimate(
            flops=4 * nk * t * r * f, bytes_accessed=20_000_000, transcendentals=t * f
        ),
        name="step",
    )(tab, rate, tokens, own, cot, received, *gathered)


def swap_core(x):
    return lax.ppermute(x, "c", [(0, 1), (1, 0)])


def swap_column(x):
    return lax.ppermute(x, "yl", [(0, 1), (1, 0)])


def partner_rows(shard, core):
    half = shard.shape[0] // 2
    return swap_core(lax.dynamic_slice_in_dim(shard, (1 - core) * half, half, axis=0))


def scatter(slots):
    return lax.psum_scatter(slots, "z", scatter_dimension=0, tiled=True)


def gather(mine):
    return lax.all_gather(mine, "z", axis=0, tiled=True)


def ring(piece, behind):
    up = [(z, (z + 1) % NZ) for z in range(NZ)]
    down = [(z, (z - 1) % NZ) for z in range(NZ)]
    low = high = piece
    pieces = [piece]
    for n in range(NZ // 2 - 1):
        low, high = lax.ppermute(low, "z", up), lax.ppermute(high, "z", down)
        if n == 1:
            low, high, behind = lax.optimization_barrier((low, high, behind))
        pieces += [low, high]
    half = piece.shape[0] // 2
    last = lax.ppermute(low[:half], "z", up), lax.ppermute(high[half:], "z", down)
    return pieces + [jnp.concatenate(last)], behind


def local(tokens, weight, momentum, cotangent, assignment, lr_index, rates):
    core = lax.axis_index("c")
    me = lax.axis_index(POP)
    partner = me + 1 - 2 * core
    loser_ids, winner_ids = assignment[:, 0], assignment[:, 1]
    win_a, win_b = jnp.min(winner_ids), jnp.max(winner_ids)

    def slot_of(member):
        hit = loser_ids == member
        return jnp.any(hit), jnp.any(hit & (winner_ids == win_b)).astype(jnp.int32)

    loser, slot = slot_of(me)
    _, partner_slot = slot_of(partner)
    tab = jnp.stack(
        [
            (win_a == me).astype(jnp.int32),
            (win_b == me).astype(jnp.int32),
            (win_a == partner).astype(jnp.int32),
            (win_b == partner).astype(jnp.int32),
            core.astype(jnp.int32),
            loser.astype(jnp.int32),
            slot,
            lax.axis_index("z").astype(jnp.int32),
        ]
    )
    member_ids = jnp.arange(lr_index.shape[0], dtype=jnp.int32)
    my_index = jnp.sum(jnp.where(member_ids == me, lr_index, 0))
    rate_ids = jnp.arange(rates.shape[0], dtype=jnp.int32)
    rate = jnp.sum(jnp.where(rate_ids == my_index, rates, 0.0)).reshape(1)

    w, m = weight[0], momentum[0]
    w_slots = build_row_slots(tab, w, partner_rows(w, core))
    w_mine = scatter(w_slots)
    own_columns = lax.all_to_all(column_blocks(w), TP, 0, 0, tiled=True)
    m_slots = build_slots(tab, m, partner_rows(m, core))
    w_mine, own_columns, m_slots, rate = lax.optimization_barrier(
        (w_mine, own_columns, m_slots, rate)
    )
    m_mine = scatter(m_slots)
    both = jnp.broadcast_to(w_mine, (2,) + w_mine.shape[1:])
    both = both.reshape((2 * NK,) + w_mine.shape[2:])
    both = lax.all_to_all(both, ("yl",) + TP, 0, 0, tiled=True)
    w_mine = both[:NK] + both[NK:]
    turned = jnp.swapaxes(tokens, 1, 2)
    w_mine, turned = lax.optimization_barrier((w_mine, turned))
    all_tokens = lax.all_to_all(
        jnp.broadcast_to(turned, (NK,) + turned.shape[1:]), TP, 0, 0, tiled=True
    )
    pieces, (m_mine, all_tokens) = ring(w_mine, (m_mine, all_tokens))
    m_across = swap_column(m_mine)
    w_other = swap_core(
        jnp.stack(
            [lax.dynamic_index_in_dim(p, partner_slot, axis=1, keepdims=False) for p in pieces]
        )
    )
    m_across, w_other = lax.optimization_barrier((m_across, w_other))
    m_won = gather(m_mine + m_across)
    activation, back = step(tab, rate, all_tokens, own_columns, cotangent[0], w_other, pieces)
    back = lax.all_to_all(back, TP, 0, 0, tiled=True)
    m_other = swap_core(lax.dynamic_index_in_dim(m_won, partner_slot, axis=1, keepdims=False))
    updated = final(tab, rate, m, m_won, m_other, back)
    return (activation[None], updated[None])


def solution(mesh):
    fine = Mesh(mesh.devices.reshape(8, 2, 2, 2, 4), POP + TP)
    placed = (
        P(POP, None, TP),
        P(POP, TP, None),
        P(POP, TP, None),
        P(POP, None, TP),
        P(),
        P(),
        P(),
    )
    return jax.shard_map(
        local,
        mesh=fine,
        in_specs=placed,
        out_specs=(P(POP, None, TP), P(POP, TP, None)),
        check_vma=False,
    )
```

```python
import jax
import jax.numpy as jnp
from jax import lax
from jax.experimental import pallas as pl
from jax.experimental.pallas import tpu as pltpu
from jax.sharding import Mesh, PartitionSpec as P

POP = ("z", "yl", "c")
TP = ("yh", "x")
NZ = 8
NK = 8
ROWS = 16
PAIR = 2
GELU_A = 0.7978845608028654
GELU_B = 0.044715

MINE_A, MINE_B, THEIRS_A, THEIRS_B, CORE, LOSER, SLOT, PLANE = range(8)
DISTANCES = (0, -1, 1, -2, 2, -3, 3, 4)


def params(n=1):
    return pltpu.CompilerParams(
        dimension_semantics=("arbitrary",) * n, vmem_limit_bytes=48 * 1024 * 1024
    )


def slots_kernel(tab, mine, theirs, out):
    pair, _, half, width = out.shape
    zero = jnp.zeros((half, width), mine.dtype)
    for j in range(pair):
        at = slice(j * width, (j + 1) * width)
        for s, (own, other) in enumerate(((MINE_A, THEIRS_A), (MINE_B, THEIRS_B))):
            out[j, s] = jnp.where(
                tab[own] == 1, mine[:, at], jnp.where(tab[other] == 1, theirs[:, at], zero)
            )


def build_slots(tab, shard, theirs):
    half, width = shard.shape[0] // 2, shard.shape[1] // NZ
    return pl.pallas_call(
        slots_kernel,
        grid_spec=pltpu.PrefetchScalarGridSpec(
            num_scalar_prefetch=1,
            grid=(NZ // PAIR,),
            in_specs=[
                pl.BlockSpec((half, PAIR * width), lambda j, tab: (tab[CORE], j)),
                pl.BlockSpec((half, PAIR * width), lambda j, tab: (0, j)),
            ],
            out_specs=pl.BlockSpec((PAIR, 2, half, width), lambda j, tab: (j, 0, 0, 0)),
        ),
        out_shape=jax.ShapeDtypeStruct((NZ, 2, half, width), shard.dtype),
        compiler_params=params(),
        cost_estimate=pl.CostEstimate(flops=5_000_000, bytes_accessed=10_000_000, transcendentals=0),
        name="slots",
    )(tab, shard, theirs)


def row_slots_kernel(tab, mine, theirs, out):
    nz, pair, _, rows, width = out.shape
    zero = jnp.zeros((rows, width), out.dtype)
    for k in range(pair):
        for z in range(nz - 1):
            at = slice(z * rows, (z + 1) * rows), slice(k * width, (k + 1) * width)
            for s, (own, other) in enumerate(((MINE_A, THEIRS_A), (MINE_B, THEIRS_B))):
                out[z, k, s] = jnp.where(
                    tab[own] == 1, mine[at], jnp.where(tab[other] == 1, theirs[at], zero)
                )
        for s in range(2):
            out[nz - 1, k, s] = zero


def build_row_slots(tab, shard, theirs):
    half, width = shard.shape[0] // 2, shard.shape[1] // NK
    rows = half // (NZ - 1)
    return pl.pallas_call(
        row_slots_kernel,
        grid_spec=pltpu.PrefetchScalarGridSpec(
            num_scalar_prefetch=1,
            grid=(NK // PAIR,),
            in_specs=[
                pl.BlockSpec((half, PAIR * width), lambda j, tab: (tab[CORE], j)),
                pl.BlockSpec((half, PAIR * width), lambda j, tab: (0, j)),
            ],
            out_specs=pl.BlockSpec((NZ, PAIR, 2, rows, width), lambda j, tab: (0, j, 0, 0, 0)),
        ),
        out_shape=jax.ShapeDtypeStruct((NZ, NK, 2, rows, width), shard.dtype),
        compiler_params=params(),
        cost_estimate=pl.CostEstimate(flops=5_000_000, bytes_accessed=10_000_000, transcendentals=0),
        name="row_slots",
    )(tab, shard, theirs)


def copy_kernel(x, out):
    width = out.shape[2]
    for k in range(out.shape[0]):
        out[k] = x[:, k * width : (k + 1) * width]


def column_blocks(shard):
    rows, width = shard.shape[0], shard.shape[1] // NK
    return pl.pallas_call(
        copy_kernel,
        grid=(NK // 2,),
        in_specs=[pl.BlockSpec((rows, 2 * width), lambda j: (0, j))],
        out_specs=pl.BlockSpec((2, rows, width), lambda j: (j, 0, 0)),
        out_shape=jax.ShapeDtypeStruct((NK, rows, width), shard.dtype),
        compiler_params=params(),
        cost_estimate=pl.CostEstimate(flops=1_000_000, bytes_accessed=6_400_000, transcendentals=0),
        name="column_blocks",
    )(shard)


def final_kernel(tab, rate, own, gathered, received, back, out):
    half, width = received.shape[1:]
    scale = 0.9 * rate[0]
    loser, first = tab[LOSER] == 1, tab[CORE] == 0

    def rows_of(at, low):
        def body(i, carry):
            here = pl.ds(pl.multiple_of(i * ROWS, ROWS), ROWS)
            there = pl.ds(pl.multiple_of(at + i * ROWS, ROWS), ROWS)
            for j in range(PAIR):
                at_j = pl.ds(j * width, width)
                g, r = gathered[j, 0, here], received[j, here]
                m = jnp.where(loser, jnp.where(low, g, r), own[there, at_j]).astype(jnp.float32)
                out[there, at_j] = (back[j, there].astype(jnp.float32) - scale * m).astype(out.dtype)
            return carry

        lax.fori_loop(0, half // ROWS, body, 0, unroll=True)

    rows_of(0, first)
    rows_of(half, jnp.logical_not(first))


def final(tab, rate, shard, gathered, received, back):
    rows, width = shard.shape[0], shard.shape[1] // NZ
    half = rows // 2
    return pl.pallas_call(
        final_kernel,
        grid_spec=pltpu.PrefetchScalarGridSpec(
            num_scalar_prefetch=2,
            grid=(NZ // PAIR,),
            in_specs=[
                pl.BlockSpec((rows, PAIR * width), lambda j, tab, rate: (0, j)),
                pl.BlockSpec((PAIR, 1, half, width), lambda j, tab, rate: (j, tab[SLOT], 0, 0)),
                pl.BlockSpec((PAIR, half, width), lambda j, tab, rate: (j, 0, 0)),
                pl.BlockSpec((PAIR, rows, width), lambda j, tab, rate: (j, 0, 0)),
            ],
            out_specs=pl.BlockSpec((rows, PAIR * width), lambda j, tab, rate: (0, j)),
        ),
        out_shape=jax.ShapeDtypeStruct(shard.shape, shard.dtype),
        compiler_params=params(),
        cost_estimate=pl.CostEstimate(flops=5_000_000, bytes_accessed=13_000_000, transcendentals=0),
        name="final",
    )(tab, rate, shard, gathered, received, back)


def step_kernel(tab, rate, tokens, own, cot, received, *refs):
    gathered, (act, back, acc, grad, weight) = refs[: len(DISTANCES)], refs[len(DISTANCES) :]
    i = pl.program_id(0)
    steps = NK // PAIR
    pair = lax.rem(i, steps) * PAIR
    half = own.shape[1] // 2
    width = own.shape[2]

    @pl.when(i < steps)
    def _():
        weight[pl.ds(pair, PAIR)] = own[...]
        for n, distance in enumerate(DISTANCES):
            plane = lax.rem(tab[PLANE] + NZ + distance, NZ)

            @pl.when((tab[LOSER] == 1) & (plane < NZ - 1))
            def _():
                near = pl.multiple_of(tab[CORE] * half + plane * ROWS, ROWS)
                far = pl.multiple_of((1 - tab[CORE]) * half + plane * ROWS, ROWS)
                for p in range(PAIR):
                    weight[pair + p, pl.ds(near, ROWS)] = gathered[n][p, 0]
                    weight[pair + p, pl.ds(far, ROWS)] = received[n, p]

        t = tokens[pl.ds(pair, PAIR)].reshape(PAIR * 2 * half, -1)
        w = weight[pl.ds(pair, PAIR)].reshape(PAIR * 2 * half, width)
        part = lax.dot_general(t, w, (((0,), (0,)), ((), ())), preferred_element_type=jnp.float32)

        @pl.when(i == 0)
        def _():
            acc[...] = part

        @pl.when(i > 0)
        def _():
            acc[...] += part

    @pl.when(i == steps - 1)
    def _():
        def body(c, carry):
            rows = pl.ds(pl.multiple_of(c * ROWS, ROWS), ROWS)
            v = acc[rows]
            vv = v * v
            t = jnp.tanh(v * (GELU_A + (GELU_A * GELU_B) * vv))
            up = 0.5 + 0.5 * t
            act[rows] = (v * up).astype(act.dtype)
            slope = up + v * (1.0 - t * t) * (0.5 * GELU_A + (1.5 * GELU_A * GELU_B) * vv)
            grad[rows] = (cot[rows].astype(jnp.float32) * slope).astype(grad.dtype)
            return carry

        lax.fori_loop(0, acc.shape[0] // ROWS, body, 0, unroll=2)

    @pl.when(i >= steps)
    def _():
        t = tokens[pl.ds(pair, PAIR)].reshape(PAIR * 2 * half, -1)
        gw = jnp.dot(t, grad[...], preferred_element_type=jnp.float32)
        w = weight[pl.ds(pair, PAIR)].reshape(PAIR * 2 * half, width)
        back[...] = (w.astype(jnp.float32) - rate[0] * gw).astype(back.dtype).reshape(back.shape)


def step(tab, rate, tokens, own, cot, received, gathered):
    nk, r, t = tokens.shape
    f = own.shape[2]
    pieces, rows = received.shape[0], received.shape[2]
    steps = NK // PAIR

    def at(i):
        return jnp.minimum(i, steps - 1)

    return pl.pallas_call(
        step_kernel,
        grid_spec=pltpu.PrefetchScalarGridSpec(
            num_scalar_prefetch=2,
            grid=(2 * steps,),
            in_specs=[
                pl.BlockSpec((nk, r, t), lambda i, tab, rate: (0, 0, 0)),
                pl.BlockSpec((PAIR, r, f), lambda i, tab, rate: (at(i), 0, 0)),
                pl.BlockSpec((t, f), lambda i, tab, rate: (0, 0)),
                pl.BlockSpec((pieces, PAIR, rows, f), lambda i, tab, rate: (0, at(i), 0, 0)),
            ]
            + [pl.BlockSpec((PAIR, 1, rows, f), lambda i, tab, rate: (at(i), tab[SLOT], 0, 0))] * pieces,
            out_specs=[
                pl.BlockSpec((t, f), lambda i, tab, rate: (0, 0)),
                pl.BlockSpec((PAIR, r, f), lambda i, tab, rate: (jnp.maximum(i - steps, 0), 0, 0)),
            ],
            scratch_shapes=[
                pltpu.VMEM((t, f), jnp.float32),
                pltpu.VMEM((t, f), jnp.bfloat16),
                pltpu.VMEM((nk, r, f), jnp.bfloat16),
            ],
        ),
        out_shape=[
            jax.ShapeDtypeStruct((t, f), jnp.bfloat16),
            jax.ShapeDtypeStruct((nk, r, f), jnp.bfloat16),
        ],
        compiler_params=params(),
        cost_estimate=pl.CostEstimate(
            flops=4 * nk * t * r * f, bytes_accessed=20_000_000, transcendentals=t * f
        ),
        name="step",
    )(tab, rate, tokens, own, cot, received, *gathered)


def swap_core(x):
    return lax.ppermute(x, "c", [(0, 1), (1, 0)])


def swap_column(x):
    return lax.ppermute(x, "yl", [(0, 1), (1, 0)])


def partner_rows(shard, core):
    half = shard.shape[0] // 2
    return swap_core(lax.dynamic_slice_in_dim(shard, (1 - core) * half, half, axis=0))


def scatter(slots):
    return lax.psum_scatter(slots, "z", scatter_dimension=0, tiled=True)


def gather(mine):
    return lax.all_gather(mine, "z", axis=0, tiled=True)


def ring(piece, behind):
    up = [(z, (z + 1) % NZ) for z in range(NZ)]
    down = [(z, (z - 1) % NZ) for z in range(NZ)]
    low = high = piece
    pieces = [piece]
    for n in range(NZ // 2 - 1):
        low, high = lax.ppermute(low, "z", up), lax.ppermute(high, "z", down)
        if n == 1:
            low, high, behind = lax.optimization_barrier((low, high, behind))
        pieces += [low, high]
    half = piece.shape[0] // 2
    last = lax.ppermute(low[:half], "z", up), lax.ppermute(high[half:], "z", down)
    return pieces + [jnp.concatenate(last)], behind


def local(tokens, weight, momentum, cotangent, assignment, lr_index, rates):
    core = lax.axis_index("c")
    me = lax.axis_index(POP)
    partner = me + 1 - 2 * core
    loser_ids, winner_ids = assignment[:, 0], assignment[:, 1]
    win_a, win_b = jnp.min(winner_ids), jnp.max(winner_ids)

    def slot_of(member):
        hit = loser_ids == member
        return jnp.any(hit), jnp.any(hit & (winner_ids == win_b)).astype(jnp.int32)

    loser, slot = slot_of(me)
    _, partner_slot = slot_of(partner)
    tab = jnp.stack(
        [
            (win_a == me).astype(jnp.int32),
            (win_b == me).astype(jnp.int32),
            (win_a == partner).astype(jnp.int32),
            (win_b == partner).astype(jnp.int32),
            core.astype(jnp.int32),
            loser.astype(jnp.int32),
            slot,
            lax.axis_index("z").astype(jnp.int32),
        ]
    )
    member_ids = jnp.arange(lr_index.shape[0], dtype=jnp.int32)
    my_index = jnp.sum(jnp.where(member_ids == me, lr_index, 0))
    rate_ids = jnp.arange(rates.shape[0], dtype=jnp.int32)
    rate = jnp.sum(jnp.where(rate_ids == my_index, rates, 0.0)).reshape(1)

    w, m = weight[0], momentum[0]
    w_slots = build_row_slots(tab, w, partner_rows(w, core))
    w_mine = scatter(w_slots)
    own_columns = lax.all_to_all(column_blocks(w), TP, 0, 0, tiled=True)
    m_slots = build_slots(tab, m, partner_rows(m, core))
    w_mine, own_columns, m_slots, rate = lax.optimization_barrier(
        (w_mine, own_columns, m_slots, rate)
    )
    m_mine = scatter(m_slots)
    both = jnp.broadcast_to(w_mine, (2,) + w_mine.shape[1:])
    both = both.reshape((2 * NK,) + w_mine.shape[2:])
    both = lax.all_to_all(both, ("yl",) + TP, 0, 0, tiled=True)
    w_mine = both[:NK] + both[NK:]
    turned = jnp.swapaxes(tokens, 1, 2)
    w_mine, turned = lax.optimization_barrier((w_mine, turned))
    all_tokens = lax.all_to_all(
        jnp.broadcast_to(turned, (NK,) + turned.shape[1:]), TP, 0, 0, tiled=True
    )
    pieces, (m_mine, all_tokens) = ring(w_mine, (m_mine, all_tokens))
    m_across = swap_column(m_mine)
    pieces[-1], m_across = lax.optimization_barrier((pieces[-1], m_across))
    w_other = swap_core(
        jnp.stack(
            [lax.dynamic_index_in_dim(p, partner_slot, axis=1, keepdims=False) for p in pieces]
        )
    )
    m_won = gather(m_mine + m_across)
    activation, back = step(tab, rate, all_tokens, own_columns, cotangent[0], w_other, pieces)
    back = lax.all_to_all(back, TP, 0, 0, tiled=True)
    m_other = swap_core(lax.dynamic_index_in_dim(m_won, partner_slot, axis=1, keepdims=False))
    updated = final(tab, rate, m, m_won, m_other, back)
    return (activation[None], updated[None])


def solution(mesh):
    fine = Mesh(mesh.devices.reshape(8, 2, 2, 2, 4), POP + TP)
    placed = (
        P(POP, None, TP),
        P(POP, TP, None),
        P(POP, TP, None),
        P(POP, None, TP),
        P(),
        P(),
        P(),
    )
    return jax.shard_map(
        local,
        mesh=fine,
        in_specs=placed,
        out_specs=(P(POP, None, TP), P(POP, TP, None)),
        check_vma=False,
    )
```

```python
import jax
import jax.numpy as jnp
from jax import lax
from jax.experimental import pallas as pl
from jax.experimental.pallas import tpu as pltpu
from jax.sharding import Mesh, PartitionSpec as P

POP = ("z", "yl", "c")
TP = ("yh", "x")
NZ = 8
NK = 8
ROWS = 16
PAIR = 2
GELU_A = 0.7978845608028654
GELU_B = 0.044715

MINE_A, MINE_B, THEIRS_A, THEIRS_B, CORE, LOSER, SLOT, PLANE = range(8)
MINE_HERE, THEIRS_HERE, MINE_ACROSS, THEIRS_ACROSS, HALF_TP = range(8, 13)
DISTANCES = (0, -1, 1, -2, 2, -3, 3, 4)


def params(n=1):
    return pltpu.CompilerParams(
        dimension_semantics=("arbitrary",) * n, vmem_limit_bytes=48 * 1024 * 1024
    )


def across_kernel(tab, mine, theirs, out):
    zero = jnp.zeros(mine.shape, mine.dtype)
    out[...] = jnp.where(
        tab[MINE_ACROSS] == 1, mine[...], jnp.where(tab[THEIRS_ACROSS] == 1, theirs[...], zero)
    )


def here_kernel(tab, mine, theirs, crossed, out):
    width = out.shape[2]
    for j in range(out.shape[0]):
        at = slice(j * width, (j + 1) * width)
        out[j] = jnp.where(
            tab[MINE_HERE] == 1,
            mine[:, at],
            jnp.where(tab[THEIRS_HERE] == 1, theirs[:, at], crossed[:, at]),
        )


def one_slot(kernel, tab, shard, halves, out_spec, out_shape, name):
    half, width = shard.shape[0] // 2, PAIR * shard.shape[1] // NZ
    return pl.pallas_call(
        kernel,
        grid_spec=pltpu.PrefetchScalarGridSpec(
            num_scalar_prefetch=1,
            grid=(NZ // PAIR,),
            in_specs=[pl.BlockSpec((half, width), lambda j, tab: (tab[CORE], j))]
            + [pl.BlockSpec((half, width), lambda j, tab: (0, j))] * len(halves),
            out_specs=out_spec,
        ),
        out_shape=jax.ShapeDtypeStruct(out_shape, shard.dtype),
        compiler_params=params(),
        cost_estimate=pl.CostEstimate(flops=2_000_000, bytes_accessed=5_000_000, transcendentals=0),
        name=name,
    )(tab, shard, *halves)


def slot_across(tab, shard, theirs):
    half, width = shard.shape[0] // 2, PAIR * shard.shape[1] // NZ
    spec = pl.BlockSpec((half, width), lambda j, tab: (0, j))
    return one_slot(across_kernel, tab, shard, (theirs,), spec, (half, shard.shape[1]), "across")


def slot_here(tab, shard, theirs, crossed):
    half, width = shard.shape[0] // 2, shard.shape[1] // NZ
    spec = pl.BlockSpec((PAIR, half, width), lambda j, tab: (j, 0, 0))
    return one_slot(here_kernel, tab, shard, (theirs, crossed), spec, (NZ, half, width), "here")


def row_slots_kernel(tab, mine, theirs, out):
    nz, pair, _, rows, width = out.shape
    zero = jnp.zeros((rows, width), out.dtype)
    for k in range(pair):
        for z in range(nz - 1):
            at = slice(z * rows, (z + 1) * rows), slice(k * width, (k + 1) * width)
            for s, (own, other) in enumerate(((MINE_A, THEIRS_A), (MINE_B, THEIRS_B))):
                out[z, k, s] = jnp.where(
                    tab[own] == 1, mine[at], jnp.where(tab[other] == 1, theirs[at], zero)
                )
        for s in range(2):
            out[nz - 1, k, s] = zero


def build_row_slots(tab, shard, theirs):
    half, width = shard.shape[0] // 2, shard.shape[1] // NK
    rows = half // (NZ - 1)
    return pl.pallas_call(
        row_slots_kernel,
        grid_spec=pltpu.PrefetchScalarGridSpec(
            num_scalar_prefetch=1,
            grid=(NK // PAIR,),
            in_specs=[
                pl.BlockSpec((half, PAIR * width), lambda j, tab: (tab[CORE], j)),
                pl.BlockSpec((half, PAIR * width), lambda j, tab: (0, j)),
            ],
            out_specs=pl.BlockSpec((NZ, PAIR, 2, rows, width), lambda j, tab: (0, j, 0, 0, 0)),
        ),
        out_shape=jax.ShapeDtypeStruct((NZ, NK, 2, rows, width), shard.dtype),
        compiler_params=params(),
        cost_estimate=pl.CostEstimate(flops=5_000_000, bytes_accessed=10_000_000, transcendentals=0),
        name="row_slots",
    )(tab, shard, theirs)


def copy_kernel(x, out):
    width = out.shape[2]
    for k in range(out.shape[0]):
        out[k] = x[:, k * width : (k + 1) * width]


def column_blocks(shard):
    rows, width = shard.shape[0], shard.shape[1] // NK
    return pl.pallas_call(
        copy_kernel,
        grid=(NK // 2,),
        in_specs=[pl.BlockSpec((rows, 2 * width), lambda j: (0, j))],
        out_specs=pl.BlockSpec((2, rows, width), lambda j: (j, 0, 0)),
        out_shape=jax.ShapeDtypeStruct((NK, rows, width), shard.dtype),
        compiler_params=params(),
        cost_estimate=pl.CostEstimate(flops=1_000_000, bytes_accessed=6_400_000, transcendentals=0),
        name="column_blocks",
    )(shard)


def final_kernel(tab, rate, own, gathered, received, back, out):
    half, width = received.shape[1:]
    scale = 0.9 * rate[0]
    loser, first = tab[LOSER] == 1, tab[CORE] == 0

    def rows_of(at, low):
        def body(i, carry):
            here = pl.ds(pl.multiple_of(i * ROWS, ROWS), ROWS)
            there = pl.ds(pl.multiple_of(at + i * ROWS, ROWS), ROWS)
            for j in range(PAIR):
                at_j = pl.ds(j * width, width)
                g, r = gathered[j, 0, here], received[j, here]
                m = jnp.where(loser, jnp.where(low, g, r), own[there, at_j]).astype(jnp.float32)
                out[there, at_j] = (back[j, there].astype(jnp.float32) - scale * m).astype(out.dtype)
            return carry

        lax.fori_loop(0, half // ROWS, body, 0, unroll=True)

    rows_of(0, first)
    rows_of(half, jnp.logical_not(first))


def final(tab, rate, shard, gathered, received, back):
    rows, width = shard.shape[0], shard.shape[1] // NZ
    half = rows // 2
    return pl.pallas_call(
        final_kernel,
        grid_spec=pltpu.PrefetchScalarGridSpec(
            num_scalar_prefetch=2,
            grid=(NZ // PAIR,),
            in_specs=[
                pl.BlockSpec((rows, PAIR * width), lambda j, tab, rate: (0, j)),
                pl.BlockSpec((PAIR, 1, half, width), lambda j, tab, rate: (j, tab[SLOT], 0, 0)),
                pl.BlockSpec((PAIR, half, width), lambda j, tab, rate: (j, 0, 0)),
                pl.BlockSpec((PAIR, rows, width), lambda j, tab, rate: (j, 0, 0)),
            ],
            out_specs=pl.BlockSpec((rows, PAIR * width), lambda j, tab, rate: (0, j)),
        ),
        out_shape=jax.ShapeDtypeStruct(shard.shape, shard.dtype),
        compiler_params=params(),
        cost_estimate=pl.CostEstimate(flops=5_000_000, bytes_accessed=13_000_000, transcendentals=0),
        name="final",
    )(tab, rate, shard, gathered, received, back)


def step_kernel(tab, rate, tokens, own, cot, received, *refs):
    gathered, (act, back, acc, grad, weight) = refs[: len(DISTANCES)], refs[len(DISTANCES) :]
    i = pl.program_id(0)
    steps = NK // PAIR
    pair = lax.rem(i, steps) * PAIR
    near_k = lax.rem(pair + (NK // 2) * tab[HALF_TP], NK)
    half = own.shape[1] // 2
    width = own.shape[2]

    @pl.when(i < steps)
    def _():
        weight[pl.ds(pair, PAIR)] = own[...]
        for n, distance in enumerate(DISTANCES):
            plane = lax.rem(tab[PLANE] + NZ + distance, NZ)

            @pl.when((tab[LOSER] == 1) & (plane < NZ - 1))
            def _():
                near = pl.multiple_of(tab[CORE] * half + plane * ROWS, ROWS)
                far = pl.multiple_of((1 - tab[CORE]) * half + plane * ROWS, ROWS)
                for p in range(PAIR):
                    weight[pair + p, pl.ds(near, ROWS)] = gathered[n][p, 0]
                    weight[pair + p, pl.ds(far, ROWS)] = received[n, p]

        t = tokens[pl.ds(near_k, PAIR)].reshape(PAIR * 2 * half, -1)
        w = weight[pl.ds(pair, PAIR)].reshape(PAIR * 2 * half, width)
        part = lax.dot_general(t, w, (((0,), (0,)), ((), ())), preferred_element_type=jnp.float32)

        @pl.when(i == 0)
        def _():
            acc[...] = part

        @pl.when(i > 0)
        def _():
            acc[...] += part

    @pl.when(i == steps - 1)
    def _():
        def body(c, carry):
            rows = pl.ds(pl.multiple_of(c * ROWS, ROWS), ROWS)
            v = acc[rows]
            vv = v * v
            t = jnp.tanh(v * (GELU_A + (GELU_A * GELU_B) * vv))
            up = 0.5 + 0.5 * t
            act[rows] = (v * up).astype(act.dtype)
            slope = up + v * (1.0 - t * t) * (0.5 * GELU_A + (1.5 * GELU_A * GELU_B) * vv)
            grad[rows] = (cot[rows].astype(jnp.float32) * slope).astype(grad.dtype)
            return carry

        lax.fori_loop(0, acc.shape[0] // ROWS, body, 0, unroll=2)

    @pl.when(i >= steps)
    def _():
        t = tokens[pl.ds(near_k, PAIR)].reshape(PAIR * 2 * half, -1)
        gw = jnp.dot(t, grad[...], preferred_element_type=jnp.float32)
        w = weight[pl.ds(pair, PAIR)].reshape(PAIR * 2 * half, width)
        back[...] = (w.astype(jnp.float32) - rate[0] * gw).astype(back.dtype).reshape(back.shape)


def step(tab, rate, tokens, own, cot, received, gathered):
    nk, r, t = tokens.shape
    f = own.shape[2]
    pieces, rows = received.shape[0], received.shape[2]
    steps = NK // PAIR

    def at(i):
        return jnp.minimum(i, steps - 1)

    return pl.pallas_call(
        step_kernel,
        grid_spec=pltpu.PrefetchScalarGridSpec(
            num_scalar_prefetch=2,
            grid=(2 * steps,),
            in_specs=[
                pl.BlockSpec((nk, r, t), lambda i, tab, rate: (0, 0, 0)),
                pl.BlockSpec((PAIR, r, f), lambda i, tab, rate: (at(i), 0, 0)),
                pl.BlockSpec((t, f), lambda i, tab, rate: (0, 0)),
                pl.BlockSpec((pieces, PAIR, rows, f), lambda i, tab, rate: (0, at(i), 0, 0)),
            ]
            + [pl.BlockSpec((PAIR, 1, rows, f), lambda i, tab, rate: (at(i), tab[SLOT], 0, 0))] * pieces,
            out_specs=[
                pl.BlockSpec((t, f), lambda i, tab, rate: (0, 0)),
                pl.BlockSpec((PAIR, r, f), lambda i, tab, rate: (jnp.maximum(i - steps, 0), 0, 0)),
            ],
            scratch_shapes=[
                pltpu.VMEM((t, f), jnp.float32),
                pltpu.VMEM((t, f), jnp.bfloat16),
                pltpu.VMEM((nk, r, f), jnp.bfloat16),
            ],
        ),
        out_shape=[
            jax.ShapeDtypeStruct((t, f), jnp.bfloat16),
            jax.ShapeDtypeStruct((nk, r, f), jnp.bfloat16),
        ],
        compiler_params=params(),
        cost_estimate=pl.CostEstimate(
            flops=4 * nk * t * r * f, bytes_accessed=20_000_000, transcendentals=t * f
        ),
        name="step",
    )(tab, rate, tokens, own, cot, received, *gathered)


def swap_core(x):
    return lax.ppermute(x, "c", [(0, 1), (1, 0)])


def swap_column(x):
    return lax.ppermute(x, "yl", [(0, 1), (1, 0)])


def partner_rows(shard, core):
    half = shard.shape[0] // 2
    return swap_core(lax.dynamic_slice_in_dim(shard, (1 - core) * half, half, axis=0))


def scatter(slots):
    return lax.psum_scatter(slots, "z", scatter_dimension=0, tiled=True)


def gather(mine):
    return lax.all_gather(mine, "z", axis=0, tiled=True)


def ring(piece, behind):
    up = [(z, (z + 1) % NZ) for z in range(NZ)]
    down = [(z, (z - 1) % NZ) for z in range(NZ)]
    low = high = piece
    pieces = [piece]
    for n in range(NZ // 2 - 1):
        low, high = lax.ppermute(low, "z", up), lax.ppermute(high, "z", down)
        if n == 1:
            low, high, behind = lax.optimization_barrier((low, high, behind))
        pieces += [low, high]
    half = piece.shape[0] // 2
    last = lax.ppermute(low[:half], "z", up), lax.ppermute(high[half:], "z", down)
    return pieces + [jnp.concatenate(last)], behind


def local(tokens, weight, momentum, cotangent, assignment, lr_index, rates):
    core = lax.axis_index("c")
    me = lax.axis_index(POP)
    partner = me + 1 - 2 * core
    loser_ids, winner_ids = assignment[:, 0], assignment[:, 1]
    win_a, win_b = jnp.min(winner_ids), jnp.max(winner_ids)
    left = lax.axis_index("yl") == 0
    here, across = jnp.where(left, win_a, win_b), jnp.where(left, win_b, win_a)

    def slot_of(member):
        hit = loser_ids == member
        return jnp.any(hit), jnp.any(hit & (winner_ids == win_b)).astype(jnp.int32)

    loser, slot = slot_of(me)
    _, partner_slot = slot_of(partner)
    tab = jnp.stack(
        [
            (win_a == me).astype(jnp.int32),
            (win_b == me).astype(jnp.int32),
            (win_a == partner).astype(jnp.int32),
            (win_b == partner).astype(jnp.int32),
            core.astype(jnp.int32),
            loser.astype(jnp.int32),
            slot,
            lax.axis_index("z").astype(jnp.int32),
            (here == me).astype(jnp.int32),
            (here == partner).astype(jnp.int32),
            (across == me).astype(jnp.int32),
            (across == partner).astype(jnp.int32),
            lax.axis_index("yh").astype(jnp.int32),
        ]
    )
    member_ids = jnp.arange(lr_index.shape[0], dtype=jnp.int32)
    my_index = jnp.sum(jnp.where(member_ids == me, lr_index, 0))
    rate_ids = jnp.arange(rates.shape[0], dtype=jnp.int32)
    rate = jnp.sum(jnp.where(rate_ids == my_index, rates, 0.0)).reshape(1)

    w, m = weight[0], momentum[0]
    w_slots = build_row_slots(tab, w, partner_rows(w, core))
    w_mine = scatter(w_slots)
    m, tokens, w_slots = lax.optimization_barrier((m, tokens, w_slots))
    m_theirs = partner_rows(m, core)
    m_cross = slot_across(tab, m, m_theirs)
    m_cross, tokens = lax.optimization_barrier((m_cross, tokens))
    turned = jnp.swapaxes(tokens, 1, 2)
    turned = jnp.broadcast_to(turned, (NK // 2,) + turned.shape[1:])
    near_tokens = lax.all_to_all(turned, "x", 0, 0, tiled=True)
    m_slot = slot_here(tab, m, m_theirs, swap_column(m_cross))
    w_blocks = column_blocks(w)
    w_mine, m_slot, w_blocks, near_tokens, rate = lax.optimization_barrier(
        (w_mine, m_slot, w_blocks, near_tokens, rate)
    )
    m_mine = scatter(m_slot)[0]
    both = jnp.broadcast_to(w_mine, (2,) + w_mine.shape[1:])
    both = both.reshape((2 * NK,) + w_mine.shape[2:])
    both = lax.all_to_all(both, ("yl",) + TP, 0, 0, tiled=True)
    w_mine = both[:NK] + both[NK:]
    w_mine, w_blocks, near_tokens = lax.optimization_barrier((w_mine, w_blocks, near_tokens))
    own_columns = lax.all_to_all(w_blocks, TP, 0, 0, tiled=True)
    far_tokens = lax.ppermute(near_tokens, "yh", [(0, 1), (1, 0)])
    pieces, m_mine = ring(w_mine, m_mine)

    m_across = swap_column(m_mine)
    pieces[-1], own_columns, far_tokens, m_across = lax.optimization_barrier(
        (pieces[-1], own_columns, far_tokens, m_across)
    )
    all_tokens = jnp.concatenate([near_tokens, far_tokens])
    w_other = swap_core(
        jnp.stack(
            [lax.dynamic_index_in_dim(p, partner_slot, axis=1, keepdims=False) for p in pieces]
        )
    )
    m_mine = jnp.where(left, jnp.stack([m_mine, m_across]), jnp.stack([m_across, m_mine]))
    m_won = gather(m_mine[None])
    activation, back = step(tab, rate, all_tokens, own_columns, cotangent[0], w_other, pieces)
    back = lax.all_to_all(back, TP, 0, 0, tiled=True)
    m_other = swap_core(lax.dynamic_index_in_dim(m_won, partner_slot, axis=1, keepdims=False))
    updated = final(tab, rate, m, m_won, m_other, back)
    return (activation[None], updated[None])


def solution(mesh):
    fine = Mesh(mesh.devices.reshape(8, 2, 2, 2, 4), POP + TP)
    placed = (
        P(POP, None, TP),
        P(POP, TP, None),
        P(POP, TP, None),
        P(POP, None, TP),
        P(),
        P(),
        P(),
    )
    return jax.shard_map(
        local,
        mesh=fine,
        in_specs=placed,
        out_specs=(P(POP, None, TP), P(POP, TP, None)),
        check_vma=False,
    )
```
